256 devices in a mesh: ta: 8 (over y, z_lo), gx: 8 (over x, core), gy: 4 (over z_hi).
Axes of the slice: x: 4, y: 4, z: 8 (z_hi: 4, z_lo: 2; z = z_hi * 2 + z_lo), core: 2. Of those that a mesh axis runs over, the one named last changes fastest.
Arguments:
- propagator: bfloat16 [8, 2, 4, 3, 4, 3, 64, 4096], P('ta', None, None, None, None, None, 'gx', 'gy'), may hold values from -1.5 to 1.5
- gamma_table: int32 [16, 8], replicated, may hold values from 0 to 3, as said below
Outputs:
- spectrum: float32 [8, 16, 64, 64, 128], P('ta', None, ('gx', 'gy'))
The draws below stay inside these ranges and needn't reach their ends.
Inputs may be any that keep to these rules, and one draw needn't show every extreme that they name: gamma_table[g, 0:4] is a permutation of 0 to 3, gamma_table[g, 4:8] are powers of i.
All inputs are finite; a program needn't handle non-finite values.
Results may differ from the reference program's by a relative error of at most 0.0061.
Values may be sent and summed in bfloat16 or wider, within the bound.
A program may use at most 192 MiB of HBM per device.

```python
import math
import jax
import jax.numpy as jnp
from jax import lax

EXTENT = 64
CHANNELS = 16
SLICES = 8


def draw_gamma_table(key, part):
    subkeys = jax.random.split(key, CHANNELS)
    orders = jax.vmap(lambda subkey: jax.random.permutation(subkey, 4))(subkeys)
    phase_codes = jax.random.randint(jax.random.fold_in(key, 11), (CHANNELS, 4), 0, 4, dtype=jnp.int32)
    return jnp.concatenate([orders.astype(jnp.int32), phase_codes], axis=1)


def level_of(stream_key, extent, cuts, low, high):
    factor_of, own = 1.0, jax.random.fold_in(stream_key, 6)
    for position, blocks in cuts:
        steps = jnp.exp(jax.random.uniform(jax.random.fold_in(own, position), (blocks,), jnp.float32, low / len(cuts), high / len(cuts)))
        factor_of = factor_of * jnp.repeat(steps, extent[position] // blocks).reshape([-1 if axis == position else 1 for axis in range(len(extent))])
    return factor_of


def bell_draw(key, shape, deviation, reach, pieces=(), kind=jnp.bfloat16):
    factor_of = level_of(key, shape, pieces, -0.22, 0.18) if pieces else 1.0
    array = jax.random.normal(key, shape, jnp.float32) * deviation * factor_of
    return jnp.minimum(jnp.maximum(array, -reach), reach).astype(kind)


def setup_inputs(seed: int = 0) -> dict:
    key_of = jax.random.split(jax.random.key(seed), 3)
    propagator = bell_draw(key_of[0], (SLICES, 2, 4, 3, 4, 3, EXTENT, EXTENT * EXTENT), 0.25, 1.5, ((0, 8), (6, 8), (7, 4)))
    gamma_table = draw_gamma_table(jax.random.fold_in(key_of[2], 71), 0)
    return dict(propagator=propagator, gamma_table=gamma_table)


def precise_dot(left_matrix, right_matrix):
    return jnp.dot(left_matrix, right_matrix, precision=lax.Precision.HIGHEST, preferred_element_type=jnp.float32)

def channel_weights(channel_table):
    spin_index = jnp.arange(4, dtype=jnp.int32)
    targets = channel_table[:, :4]
    codes_all = channel_table[:, 4:]
    mapping = (targets[:, :, None] == spin_index[None, None, :]).astype(jnp.float32)
    phase_real = (codes_all == 0).astype(jnp.float32) - (codes_all == 2).astype(jnp.float32)
    phase_imag = (codes_all == 1).astype(jnp.float32) - (codes_all == 3).astype(jnp.float32)
    pair_real = phase_real[:, None, :] * phase_real[:, :, None] - phase_imag[:, None, :] * phase_imag[:, :, None]
    pair_imag = phase_real[:, None, :] * phase_imag[:, :, None] + phase_imag[:, None, :] * phase_real[:, :, None]
    source_map = jnp.transpose(mapping, (0, 2, 1))
    selector = source_map[:, :, None, :, None] * mapping[:, None, :, None, :]
    count_channels = channel_table.shape[0]
    weight_real = (pair_real[:, None, :, :, None] * selector).reshape(count_channels, 256)
    weight_imag = (pair_imag[:, None, :, :, None] * selector).reshape(count_channels, 256)
    return (weight_real, weight_imag)

def spin_products(field_real, field_imag):
    site_count = field_real.shape[-1]
    total_real = jnp.zeros((4, 4, 4, 4, site_count), jnp.float32)
    total_imag = jnp.zeros((4, 4, 4, 4, site_count), jnp.float32)
    for color_in in range(3):
        for color_out in range(3):
            left_real = field_real[:, color_in, :, color_out].astype(jnp.float32)
            left_imag = field_imag[:, color_in, :, color_out].astype(jnp.float32)
            total_real = total_real + left_real[:, :, None, None] * left_real[None, None] + left_imag[:, :, None, None] * left_imag[None, None]
            total_imag = total_imag + left_imag[:, :, None, None] * left_real[None, None] - left_real[:, :, None, None] * left_imag[None, None]
    return (total_real.reshape(256, site_count), total_imag.reshape(256, site_count))

def dft_tables(length):
    steps_index = jnp.arange(length, dtype=jnp.int32)
    phases = steps_index[:, None] * steps_index[None, :] % length
    angles = phases.astype(jnp.float32) * (2.0 * math.pi / length)
    norm_factor = 1.0 / math.sqrt(length)
    cosine = (jnp.cos(angles) * norm_factor).astype(jnp.bfloat16)
    sine_table = (jnp.sin(angles) * norm_factor).astype(jnp.bfloat16)
    return (cosine.astype(jnp.float32), sine_table.astype(jnp.float32))

def section(complex_pair, which_axis, cosine, sine_table):
    field_real = complex_pair[0].astype(jnp.float32)
    field_imag = complex_pair[1].astype(jnp.float32)

    def contract_axis(values, weights):
        moved = jnp.tensordot(values, weights, axes=([which_axis], [0]), precision=lax.Precision.HIGHEST)
        return jnp.moveaxis(moved, -1, which_axis)
    new_real = contract_axis(field_real, cosine) + contract_axis(field_imag, sine_table)
    new_imag = contract_axis(field_imag, cosine) - contract_axis(field_real, sine_table)
    return (new_real, new_imag)

def to_half(complex_pair):
    return lax.optimization_barrier((complex_pair[0].astype(jnp.bfloat16), complex_pair[1].astype(jnp.bfloat16)))

def reference(propagator, gamma_table):
    weight_real, weight_imag = channel_weights(gamma_table)
    stack_real = jnp.concatenate([weight_real, -weight_imag], axis=1)
    stack_imag = jnp.concatenate([weight_imag, weight_real], axis=1)
    cosine, sine_table = dft_tables(EXTENT)
    volume = EXTENT ** 3

    def one_slice(slice_block):
        flattened = slice_block.astype(jnp.float32).reshape(2, 4, 3, 4, 3, volume)
        prod_real, prod_imag = spin_products(flattened[0], flattened[1])
        prod_stack = jnp.concatenate([prod_real, prod_imag], axis=0).astype(jnp.bfloat16)
        prod_stack = lax.optimization_barrier(prod_stack).astype(jnp.float32)
        dens_real = precise_dot(stack_real, prod_stack).reshape(-1, EXTENT, EXTENT, EXTENT)
        dens_imag = precise_dot(stack_imag, prod_stack).reshape(-1, EXTENT, EXTENT, EXTENT)
        pair = to_half((dens_real, dens_imag))
        pair = to_half(section(pair, 3, cosine, sine_table))
        pair = to_half(section(pair, 2, cosine, sine_table))
        spec_real, spec_imag = section(pair, 1, cosine, sine_table)
        spec_real = jnp.transpose(spec_real, (0, 3, 1, 2))
        spec_imag = jnp.transpose(spec_imag, (0, 3, 1, 2))
        return jnp.concatenate([spec_real, spec_imag], axis=3).astype(jnp.float32)
    return lax.map(one_slice, propagator)
```

```python
import functools
import math

import jax
import jax.numpy as jnp
import numpy as np
from jax import lax
from jax.experimental import pallas as pl
from jax.experimental.pallas import tpu as pltpu
from jax.sharding import PartitionSpec as P

EXTENT = 64
CHANNELS = 16
SPINS = 16
COLORS = 9
BLOCKS = 4
LANES = 256
MESH = pl.DeviceIdType.MESH
F32 = jnp.float32
BF16 = jnp.bfloat16
PAIRS = [(lo, hi) for lo in range(SPINS) for hi in range(lo + 1, SPINS)]


def slot_table():
    slots = [(lo, hi, part) for lo, hi in PAIRS for part in (0, 1)]
    slots += [(spin, spin, 0) for spin in range(SPINS)]
    columns = np.repeat(np.array(slots, np.int32), 8, axis=0)
    table = np.zeros((8, columns.shape[0]), np.int32)
    table[:3] = columns.T
    table[3] = np.arange(columns.shape[0]) % 8
    return table


def dft_tables():
    steps = np.arange(EXTENT)
    angles = (steps[:, None] * steps[None, :] % EXTENT) * (2.0 * math.pi / EXTENT)
    norm = 1.0 / math.sqrt(EXTENT)
    return np.cos(angles) * norm, np.sin(angles) * norm


def rotation(cosine, sine):
    table = np.zeros((2, EXTENT, 2, EXTENT))
    table[0, :, 0] = cosine
    table[1, :, 0] = sine
    table[0, :, 1] = -sine
    table[1, :, 1] = cosine
    return table


def weights_z():
    turn = rotation(*dft_tables())
    table = np.zeros((32, 2, 2, 2, 2, 2, EXTENT))
    for y in range(2):
        block = turn.transpose(3, 2, 0, 1).reshape(32, 2, 2, 2, EXTENT)
        table[:, :, :, y, :, y, :] = block
    return table.reshape(256, 256)


def weights_y():
    turn = rotation(*dft_tables())
    swapped = np.stack([turn[:, :, 1], -turn[:, :, 0]], axis=2)
    both = np.stack([turn, swapped], axis=2)
    both = both.reshape(2, 4, 4, 2, 2, 2, 2, EXTENT)
    table = np.zeros((4, 4, 2, 2, 2, 2, 2, 2, 2, EXTENT))
    for kz in range(2):
        table[:, :, :, kz, :, :, :, kz] = both.transpose(1, 2, 3, 0, 4, 5, 6, 7)
    return table.reshape(256, 512)


def weights_x():
    cosine, sine = dft_tables()
    return np.concatenate([cosine.T, sine.T], axis=1)


def channel_rows(gamma, table):
    lo, hi = table[0:1], table[1:2]
    imaginary = table[2:3] == 1

    def pick(base, index):
        out = jnp.zeros((CHANNELS, index.shape[1]), jnp.int32)
        for spin in range(4):
            out = jnp.where(index == spin, gamma[:, base + spin : base + spin + 1], out)
        return out

    lo_1, lo_2 = lax.div(lo, 4), lax.rem(lo, 4)
    hi_1, hi_2 = lax.div(hi, 4), lax.rem(hi, 4)
    phase = {}
    for name, (s1, s2, s3, s4) in {
        "straight": (lo_1, lo_2, hi_1, hi_2),
        "reversed": (hi_1, hi_2, lo_1, lo_2),
    }.items():
        hit = jnp.logical_and(pick(0, s3) == s1, pick(0, s2) == s4)
        turn = jnp.where(hit, lax.rem(pick(4, s3) + pick(4, s2), 4), 7)
        one, zero = jnp.float32(1), jnp.float32(0)
        real = jnp.where(turn == 0, one, zero) - jnp.where(turn == 2, one, zero)
        imag = jnp.where(turn == 1, one, zero) - jnp.where(turn == 3, one, zero)
        phase[name] = (real, imag)
    (r1, i1), (r2, i2) = phase["straight"], phase["reversed"]
    diagonal = lo == hi
    r2 = jnp.where(diagonal, 0.0, r2)
    i2 = jnp.where(diagonal, 0.0, i2)
    rows_real = jnp.where(imaginary, i2 - i1, r1 + r2)
    rows_imag = jnp.where(imaginary, r1 - r2, i1 + i2)
    return rows_real, rows_imag


def plane(part, spin, color):
    s1, s2 = divmod(spin, 4)
    c1, c2 = divmod(color, 3)
    return part * 144 + ((s1 * 3 + c1) * 4 + s2) * 3 + c2


def spin_products(field, products):
    load = lambda part, spin: [field[plane(part, spin, color)] for color in range(COLORS)]

    def chain(terms):
        total = None
        for left, right in terms:
            product = left.astype(F32) * right.astype(F32)
            total = product if total is None else total + product
        return total

    row = 0
    for lo in range(SPINS):
        lo_real, lo_imag = load(0, lo), load(1, lo)
        lo_minus = [-value for value in lo_real]
        for hi in range(lo + 1, SPINS):
            hi_real, hi_imag = load(0, hi), load(1, hi)
            real = chain([*zip(lo_real, hi_real), *zip(lo_imag, hi_imag)])
            imag = chain([*zip(lo_imag, hi_real), *zip(lo_minus, hi_imag)])
            products[row : row + 16] = jnp.concatenate([real, imag], axis=0).astype(BF16)
            row += 16
    for first in range(0, SPINS, 2):
        squares = []
        for spin in (first, first + 1):
            real, imag = load(0, spin), load(1, spin)
            squares.append(chain([*zip(real, real), *zip(imag, imag)]))
        products[row : row + 16] = jnp.concatenate(squares, axis=0).astype(BF16)
        row += 16


def peer(gx, gy, dx, dc, dy):
    core = lax.rem(gx, 2)
    to_core = core + dc - 2 * dc * core
    return lax.rem(gx // 2 + dx, 4) * 2 + to_core, lax.rem(gy + dy, 4)


def send_order():
    by_dy = {dy: [(dx, dc, dy) for dx in range(4) for dc in range(2) if (dx, dc, dy) != (0, 0, 0)] for dy in range(4)}
    order = []
    for step in range(8):
        for dy in (2, 1, 3, 0):
            if step < len(by_dy[dy]):
                order.append(by_dy[dy][step])
    return order


def front_kernel(
    prop, gamma, table, wz, received, field, weights, products, message, load_sem, send_sem, recv_sem
):
    gx, gy = lax.axis_index("gx"), lax.axis_index("gy")
    me = gx * 4 + gy
    offsets = send_order()
    loads = [
        pltpu.make_async_copy(prop.at[:, :, pl.ds(j * LANES, LANES)], field.at[j], load_sem.at[j])
        for j in range(BLOCKS)
    ]
    for load in loads:
        load.start()
    barrier = pltpu.get_barrier_semaphore()
    for offset in offsets:
        to_x, to_y = peer(gx, gy, *offset)
        pl.semaphore_signal(barrier, inc=1, device_id={"gx": to_x, "gy": to_y}, device_id_type=MESH)

    def build(tile, carry):
        at = pl.ds(pl.multiple_of(tile * LANES, LANES), LANES)
        columns = table[:, at]
        keep = lax.broadcasted_iota(jnp.int32, (8, LANES), 0) == columns[3:4]
        for c, rows in enumerate(channel_rows(gamma[...], columns)):
            for g in range(0, CHANNELS, 2):
                pair = [
                    jnp.where(keep, jnp.broadcast_to(rows[g + i : g + i + 1], (8, LANES)), 0.0)
                    for i in range(2)
                ]
                start = c * 128 + g * 8
                weights[start : start + 16, at] = jnp.concatenate(pair, axis=0).astype(BF16)
        return carry

    lax.fori_loop(0, 8, build, 0)

    for j in range(BLOCKS):
        loads[j].wait()

    def block(j, carry):
        spin_products(field.at[j], products)
        density = jnp.dot(weights[...], products[...], preferred_element_type=F32).astype(BF16)
        pieces = [
            jnp.concatenate(
                [density[:128, t * 128 : t * 128 + 128], density[128:, t * 128 : t * 128 + 128]], axis=1
            )
            for t in range(2)
        ]
        along = lax.dot_general(
            wz[...], jnp.concatenate(pieces, axis=0), (((1,), (1,)), ((), ())), preferred_element_type=F32
        )
        along = along.reshape(32, 8, LANES)
        message[j] = jnp.concatenate([along[:, :, :128], along[:, :, 128:]], axis=1).astype(BF16)

        @pl.when(j == 0)
        def _():
            pl.semaphore_wait(barrier, len(offsets))

        for offset in offsets:
            to_x, to_y = peer(gx, gy, *offset)
            pltpu.make_async_remote_copy(
                src_ref=message.at[j, to_x * 4 + to_y],
                dst_ref=received.at[me * 4 + j],
                send_sem=send_sem,
                recv_sem=recv_sem,
                device_id={"gx": to_x, "gy": to_y},
                device_id_type=MESH,
            ).start()
        received[me * 4 + j] = message[j, me]
        return carry

    lax.fori_loop(0, BLOCKS, block, 0)
    remote = pl.ds(0, 31 * BLOCKS)
    everything = received.at[remote]
    pltpu.make_async_copy(everything, everything, send_sem).wait()
    pltpu.make_async_copy(everything, everything, recv_sem).wait()


def back_kernel(received, wy, wx, out, along_y):
    for gx in range(8):
        piece = received[gx * 16 : gx * 16 + 16].reshape(256, 128)
        turned = lax.dot_general(piece, wy[...], (((0,), (0,)), ((), ())), preferred_element_type=F32)
        along_y[gx] = turned.reshape(CHANNELS, 8, 512)
    for g in range(CHANNELS):
        rows = along_y[:, g].reshape(EXTENT, 512)
        rows = jnp.concatenate([rows[:, :256], rows[:, 256:]], axis=0).astype(BF16)
        spectrum = jnp.dot(wx[...], rows, preferred_element_type=F32)
        out[g, 0] = spectrum[:, :128]
        out[g, 1] = spectrum[:, 128:]


def body(propagator, gamma_table):
    vmem = pl.BlockSpec(memory_space=pltpu.VMEM)
    prop = propagator.reshape(288, 8, 1024)
    received = pl.pallas_call(
        front_kernel,
        out_shape=jax.ShapeDtypeStruct((128, 16, 128), BF16),
        in_specs=[pl.BlockSpec(memory_space=pl.ANY), vmem, vmem, vmem],
        out_specs=vmem,
        scratch_shapes=[
            pltpu.VMEM((BLOCKS, 288, 8, LANES), BF16),
            pltpu.VMEM((256, 2048), BF16),
            pltpu.VMEM((2048, LANES), BF16),
            pltpu.VMEM((BLOCKS, 32, 16, 128), BF16),
            pltpu.SemaphoreType.DMA((BLOCKS,)),
            pltpu.SemaphoreType.DMA,
            pltpu.SemaphoreType.DMA,
        ],
        compiler_params=pltpu.CompilerParams(collective_id=0, has_side_effects=True),
    )(prop, gamma_table, jnp.asarray(slot_table()), jnp.asarray(weights_z(), BF16))
    out = pl.pallas_call(
        back_kernel,
        out_shape=jax.ShapeDtypeStruct((CHANNELS, 2, EXTENT, 128), F32),
        in_specs=[vmem, vmem, vmem],
        out_specs=vmem,
        scratch_shapes=[pltpu.VMEM((8, CHANNELS, 8, 512), F32)],
    )(received, jnp.asarray(weights_y(), BF16), jnp.asarray(weights_x(), BF16))
    return out[None]


def solution(mesh):
    return jax.shard_map(
        body,
        mesh=mesh,
        in_specs=(P("ta", None, None, None, None, None, "gx", "gy"), P()),
        out_specs=P("ta", None, ("gx", "gy"), None, None),
        check_vma=False,
    )
```

```python
import functools
import math

import jax
import jax.numpy as jnp
import numpy as np
from jax import lax
from jax.experimental import pallas as pl
from jax.experimental.pallas import tpu as pltpu
from jax.sharding import PartitionSpec as P

EXTENT = 64
CHANNELS = 16
SPINS = 16
COLORS = 9
BLOCKS = 4
LANES = 256
SERVED = (((0, 1), 0), ((3, 2), 2))
FRONT_VMEM = 20 * 2**20
BACK_VMEM = 16 * 2**20
MESH = pl.DeviceIdType.MESH
F32 = jnp.float32
BF16 = jnp.bfloat16
PAIRS = [(lo, hi) for lo in range(SPINS) for hi in range(lo + 1, SPINS)]


def slot_table():
    slots = [(lo, hi, part) for lo, hi in PAIRS for part in (0, 1)]
    slots += [(spin, spin, 0) for spin in range(SPINS)]
    columns = np.repeat(np.array(slots, np.int32), 8, axis=0)
    table = np.zeros((8, columns.shape[0]), np.int32)
    table[:3] = columns.T
    table[3] = np.arange(columns.shape[0]) % 8
    return table


def dft_tables():
    steps = np.arange(EXTENT)
    angles = (steps[:, None] * steps[None, :] % EXTENT) * (2.0 * math.pi / EXTENT)
    norm = 1.0 / math.sqrt(EXTENT)
    return np.cos(angles) * norm, np.sin(angles) * norm


def rotation(cosine, sine):
    table = np.zeros((2, EXTENT, 2, EXTENT))
    table[0, :, 0] = cosine
    table[1, :, 0] = sine
    table[0, :, 1] = -sine
    table[1, :, 1] = cosine
    return table


def weights_z():
    turn = rotation(*dft_tables())
    table = np.zeros((32, 2, 2, 2, 2, 2, EXTENT))
    for y in range(2):
        block = turn.transpose(3, 2, 0, 1).reshape(32, 2, 2, 2, EXTENT)
        table[:, :, :, y, :, y, :] = block
    return table.reshape(256, 256)


def weights_y():
    turn = rotation(*dft_tables())
    swapped = np.stack([turn[:, :, 1], -turn[:, :, 0]], axis=2)
    both = np.stack([turn, swapped], axis=2)
    both = both.reshape(2, 4, 4, 2, 2, 2, 2, EXTENT)
    table = np.zeros((4, 4, 2, 2, 2, 2, 2, 2, 2, EXTENT))
    for kz in range(2):
        table[:, :, :, kz, :, :, :, kz] = both.transpose(1, 2, 3, 0, 4, 5, 6, 7)
    return table.reshape(256, 512)


def weights_x():
    cosine, sine = dft_tables()
    return np.concatenate([cosine.T, sine.T], axis=1)


def channel_rows(gamma, table):
    lo, hi = table[0:1], table[1:2]
    imaginary = table[2:3] == 1

    def pick(base, index):
        out = jnp.zeros((CHANNELS, index.shape[1]), jnp.int32)
        for spin in range(4):
            out = jnp.where(index == spin, gamma[:, base + spin : base + spin + 1], out)
        return out

    lo_1, lo_2 = lax.div(lo, 4), lax.rem(lo, 4)
    hi_1, hi_2 = lax.div(hi, 4), lax.rem(hi, 4)
    phase = {}
    for name, (s1, s2, s3, s4) in {
        "straight": (lo_1, lo_2, hi_1, hi_2),
        "reversed": (hi_1, hi_2, lo_1, lo_2),
    }.items():
        hit = jnp.logical_and(pick(0, s3) == s1, pick(0, s2) == s4)
        turn = jnp.where(hit, lax.rem(pick(4, s3) + pick(4, s2), 4), 7)
        one, zero = jnp.float32(1), jnp.float32(0)
        real = jnp.where(turn == 0, one, zero) - jnp.where(turn == 2, one, zero)
        imag = jnp.where(turn == 1, one, zero) - jnp.where(turn == 3, one, zero)
        phase[name] = (real, imag)
    (r1, i1), (r2, i2) = phase["straight"], phase["reversed"]
    diagonal = lo == hi
    r2 = jnp.where(diagonal, 0.0, r2)
    i2 = jnp.where(diagonal, 0.0, i2)
    rows_real = jnp.where(imaginary, i2 - i1, r1 + r2)
    rows_imag = jnp.where(imaginary, r1 - r2, i1 + i2)
    return rows_real, rows_imag


def plane(part, spin, color):
    s1, s2 = divmod(spin, 4)
    c1, c2 = divmod(color, 3)
    return part * 144 + ((s1 * 3 + c1) * 4 + s2) * 3 + c2


def spin_products(field, products):
    load = lambda part, spin: [field[plane(part, spin, color)] for color in range(COLORS)]

    def chain(terms):
        total = None
        for left, right in terms:
            product = left.astype(F32) * right.astype(F32)
            total = product if total is None else total + product
        return total

    row = 0
    for lo in range(SPINS):
        lo_real, lo_imag = load(0, lo), load(1, lo)
        lo_minus = [-value for value in lo_real]
        for hi in range(lo + 1, SPINS):
            hi_real, hi_imag = load(0, hi), load(1, hi)
            real = chain([*zip(lo_real, hi_real), *zip(lo_imag, hi_imag)])
            imag = chain([*zip(lo_imag, hi_real), *zip(lo_minus, hi_imag)])
            products[row : row + 16] = jnp.concatenate([real, imag], axis=0).astype(BF16)
            row += 16
    for first in range(0, SPINS, 2):
        squares = []
        for spin in (first, first + 1):
            real, imag = load(0, spin), load(1, spin)
            squares.append(chain([*zip(real, real), *zip(imag, imag)]))
        products[row : row + 16] = jnp.concatenate(squares, axis=0).astype(BF16)
        row += 16


def peer(gx, dx, dc):
    core = lax.rem(gx, 2)
    return lax.rem(gx // 2 + dx, 4) * 2 + core + dc - 2 * dc * core


OFFSETS = [(dx, dc) for dx in (2, 1, 3, 0) for dc in (1, 0)]


def front_kernel(
    prop, gamma_hbm, table_hbm, wz_hbm, received,
    field, gamma, table, wz, weights, products, message, load_sem, small_sem, send_sem, recv_sem,
):
    gx, gy = lax.axis_index("gx"), lax.axis_index("gy")
    me = gx * 4 + gy
    barrier = pltpu.get_barrier_semaphore()

    def each_peer(rows, act):
        for dx, dc in OFFSETS:
            for to_y in rows:
                if (dx, dc) == (0, 0):
                    pl.when(gy != to_y)(functools.partial(act, gx, to_y))
                else:
                    act(peer(gx, dx, dc), to_y)

    def greet(to_x, to_y):
        pl.semaphore_signal(barrier, inc=1, device_id={"gx": to_x, "gy": to_y}, device_id_type=MESH)

    each_peer((0, 1, 2, 3), greet)
    small = [
        pltpu.make_async_copy(source, target, small_sem.at[i])
        for i, (source, target) in enumerate([(gamma_hbm, gamma), (table_hbm, table), (wz_hbm, wz)])
    ]

    def load(j):
        start = j * LANES if isinstance(j, int) else pl.multiple_of(j * LANES, LANES)
        return pltpu.make_async_copy(prop.at[:, :, pl.ds(start, LANES)], field.at[j], load_sem.at[j])

    small[0].start()
    small[1].start()
    load(0).start()
    small[2].start()
    for j in range(1, BLOCKS):
        load(j).start()
    small[0].wait()
    small[1].wait()
    rows = jnp.concatenate([gamma[...].astype(F32), jnp.zeros((8, 112), F32)], axis=1)
    rows = jnp.concatenate([rows, jnp.zeros((120, 128), F32)], axis=0)
    channels = jnp.transpose(rows)[:CHANNELS, :8].astype(jnp.int32)

    def build(tile, carry):
        at = pl.ds(pl.multiple_of(tile * LANES, LANES), LANES)
        columns = table[:, at]
        keep = lax.broadcasted_iota(jnp.int32, (8, LANES), 0) == columns[3:4]
        for c, rows in enumerate(channel_rows(channels, columns)):
            for g in range(0, CHANNELS, 2):
                pair = [
                    jnp.where(keep, jnp.broadcast_to(rows[g + i : g + i + 1], (8, LANES)), 0.0)
                    for i in range(2)
                ]
                start = c * 128 + g * 8
                weights[start : start + 16, at] = jnp.concatenate(pair, axis=0).astype(BF16)
        return carry

    lax.fori_loop(0, 8, build, 0)

    small[2].wait()

    def block(j, carry):
        load(j).wait()
        spin_products(field.at[j], products)
        density = jnp.dot(weights[...], products[...], preferred_element_type=F32).astype(BF16)
        pieces = [
            jnp.concatenate(
                [density[:128, t * 128 : t * 128 + 128], density[128:, t * 128 : t * 128 + 128]], axis=1
            )
            for t in range(2)
        ]
        along = lax.dot_general(
            wz[...], jnp.concatenate(pieces, axis=0), (((1,), (1,)), ((), ())), preferred_element_type=F32
        )
        along = along.reshape(32, 8, LANES)
        message[:, j] = jnp.concatenate([along[:, :, :128], along[:, :, 128:]], axis=1).astype(BF16)
        received[me * BLOCKS + j] = message[me, j]

        @pl.when(j == 0)
        def _():
            pl.semaphore_wait(barrier, 31)

        for rows, lag in SERVED:
            if lag == 0:
                send_block(rows, j)
            else:
                pl.when(j >= lag)(functools.partial(send_block, rows, j - lag))
        return carry

    def send(source, target, to_x, to_y):
        pltpu.make_async_remote_copy(
            src_ref=source,
            dst_ref=target,
            send_sem=send_sem,
            recv_sem=recv_sem,
            device_id={"gx": to_x, "gy": to_y},
            device_id_type=MESH,
        ).start()

    def send_block(rows, j):
        each_peer(
            rows,
            lambda to_x, to_y: send(
                message.at[to_x * 4 + to_y, j], received.at[me * BLOCKS + j], to_x, to_y
            ),
        )

    lax.fori_loop(0, BLOCKS, block, 0)
    for step in range(BLOCKS, BLOCKS + max(lag for _, lag in SERVED)):
        for rows, lag in SERVED:
            if step - lag < BLOCKS:
                send_block(rows, step - lag)
    remote = pl.ds(0, 31 * BLOCKS)
    everything = received.at[remote]
    pltpu.make_async_copy(everything, everything, send_sem).wait()
    pltpu.make_async_copy(everything, everything, recv_sem).wait()


def back_kernel(received, wy, wx, out, along_y, spectrum, out_sem):
    for gx in range(8):
        piece = received[gx * 16 : gx * 16 + 16].reshape(256, 128)
        turned = lax.dot_general(piece, wy[...], (((0,), (0,)), ((), ())), preferred_element_type=F32)
        along_y[gx] = turned.reshape(CHANNELS, 8, 512)
    for g in range(CHANNELS):
        rows = along_y[:, g].reshape(EXTENT, 512)
        rows = jnp.concatenate([rows[:, :256], rows[:, 256:]], axis=0).astype(BF16)
        both = jnp.dot(wx[...], rows, preferred_element_type=F32)
        spectrum[g, 0] = both[:, :128]
        spectrum[g, 1] = both[:, 128:]
        pltpu.make_async_copy(spectrum.at[g], out.at[g], out_sem.at[g]).start()
    for g in range(CHANNELS):
        pltpu.make_async_copy(spectrum.at[g], out.at[g], out_sem.at[g]).wait()


def body(propagator, gamma_table):
    vmem = pl.BlockSpec(memory_space=pltpu.VMEM)
    hbm = pl.BlockSpec(memory_space=pltpu.HBM)
    prop = propagator.reshape(288, 8, 1024)
    received = pl.pallas_call(
        front_kernel,
        out_shape=pltpu.VMEM((128, 16, 128), BF16),
        in_specs=[hbm, hbm, hbm, hbm],
        out_specs=vmem,
        scratch_shapes=[
            pltpu.VMEM((BLOCKS, 288, 8, LANES), BF16),
            pltpu.VMEM((8, CHANNELS), jnp.int32),
            pltpu.VMEM((8, 2048), jnp.int32),
            pltpu.VMEM((256, 256), BF16),
            pltpu.VMEM((256, 2048), BF16),
            pltpu.VMEM((2048, LANES), BF16),
            pltpu.VMEM((32, BLOCKS, 16, 128), BF16),
            pltpu.SemaphoreType.DMA((BLOCKS,)),
            pltpu.SemaphoreType.DMA((3,)),
            pltpu.SemaphoreType.DMA,
            pltpu.SemaphoreType.DMA,
        ],
        compiler_params=pltpu.CompilerParams(
            collective_id=0, has_side_effects=True, vmem_limit_bytes=FRONT_VMEM
        ),
    )(*[pltpu.with_memory_space_constraint(x, pltpu.HBM) for x in (prop, gamma_table.T, jnp.asarray(slot_table()), jnp.asarray(weights_z(), BF16))])
    out = pl.pallas_call(
        back_kernel,
        out_shape=jax.ShapeDtypeStruct((CHANNELS, 2, EXTENT, 128), F32),
        in_specs=[vmem, vmem, vmem],
        out_specs=hbm,
        scratch_shapes=[
            pltpu.VMEM((8, CHANNELS, 8, 512), F32),
            pltpu.VMEM((CHANNELS, 2, EXTENT, 128), F32),
            pltpu.SemaphoreType.DMA((CHANNELS,)),
        ],
        compiler_params=pltpu.CompilerParams(vmem_limit_bytes=BACK_VMEM),
    )(received, jnp.asarray(weights_y(), BF16), jnp.asarray(weights_x(), BF16))
    return out[None]


def solution(mesh):
    return jax.shard_map(
        body,
        mesh=mesh,
        in_specs=(P("ta", None, None, None, None, None, "gx", "gy"), P()),
        out_specs=P("ta", None, ("gx", "gy"), None, None),
        check_vma=False,
    )
```

```python
import functools
import math

import jax
import jax.numpy as jnp
import numpy as np
from jax import lax
from jax.experimental import pallas as pl
from jax.experimental.pallas import tpu as pltpu
from jax.sharding import PartitionSpec as P

EXTENT = 64
CHANNELS = 16
SPINS = 16
COLORS = 9
BLOCKS = 4
LANES = 256
EARLY, LATE = (0, 1), (3, 2)
FRONT_VMEM = 20 * 2**20
BACK_VMEM = 16 * 2**20
MESH = pl.DeviceIdType.MESH
F32 = jnp.float32
BF16 = jnp.bfloat16
PAIRS = [(lo, hi) for lo in range(SPINS) for hi in range(lo + 1, SPINS)]


def slot_table():
    slots = [(lo, hi, part) for lo, hi in PAIRS for part in (0, 1)]
    slots += [(spin, spin, 0) for spin in range(SPINS)]
    table = np.zeros((8, 256), np.int32)
    table[:3] = np.array(slots, np.int32).T
    return table


def dft_tables():
    steps = np.arange(EXTENT)
    angles = (steps[:, None] * steps[None, :] % EXTENT) * (2.0 * math.pi / EXTENT)
    norm = 1.0 / math.sqrt(EXTENT)
    return np.cos(angles) * norm, np.sin(angles) * norm


def rotation(cosine, sine):
    table = np.zeros((2, EXTENT, 2, EXTENT))
    table[0, :, 0] = cosine
    table[1, :, 0] = sine
    table[0, :, 1] = -sine
    table[1, :, 1] = cosine
    return table


def weights_z():
    turn = rotation(*dft_tables())
    table = np.zeros((32, 2, 2, 2, 2, 2, EXTENT))
    for y in range(2):
        block = turn.transpose(3, 2, 0, 1).reshape(32, 2, 2, 2, EXTENT)
        table[:, :, :, y, :, y, :] = block
    return table.reshape(256, 256)


def weights_y():
    turn = rotation(*dft_tables())
    swapped = np.stack([turn[:, :, 1], -turn[:, :, 0]], axis=2)
    both = np.stack([turn, swapped], axis=2)
    both = both.reshape(2, 4, 4, 2, 2, 2, 2, EXTENT)
    table = np.zeros((4, 4, 2, 2, 2, 2, 2, 2, 2, EXTENT))
    for kz in range(2):
        table[:, :, :, kz, :, :, :, kz] = both.transpose(1, 2, 3, 0, 4, 5, 6, 7)
    return table.reshape(256, 512)


def weights_x():
    cosine, sine = dft_tables()
    return np.concatenate([cosine.T, sine.T], axis=1)


def channel_rows(gamma, table):
    lo, hi = table[0:1], table[1:2]
    imaginary = table[2:3] == 1

    def pick(base, index):
        out = jnp.zeros((CHANNELS, index.shape[1]), jnp.int32)
        for spin in range(4):
            out = jnp.where(index == spin, gamma[:, base + spin : base + spin + 1], out)
        return out

    lo_1, lo_2 = lax.div(lo, 4), lax.rem(lo, 4)
    hi_1, hi_2 = lax.div(hi, 4), lax.rem(hi, 4)
    phase = {}
    for name, (s1, s2, s3, s4) in {
        "straight": (lo_1, lo_2, hi_1, hi_2),
        "reversed": (hi_1, hi_2, lo_1, lo_2),
    }.items():
        hit = jnp.logical_and(pick(0, s3) == s1, pick(0, s2) == s4)
        turn = jnp.where(hit, lax.rem(pick(4, s3) + pick(4, s2), 4), 7)
        one, zero = jnp.float32(1), jnp.float32(0)
        real = jnp.where(turn == 0, one, zero) - jnp.where(turn == 2, one, zero)
        imag = jnp.where(turn == 1, one, zero) - jnp.where(turn == 3, one, zero)
        phase[name] = (real, imag)
    (r1, i1), (r2, i2) = phase["straight"], phase["reversed"]
    diagonal = lo == hi
    r2 = jnp.where(diagonal, 0.0, r2)
    i2 = jnp.where(diagonal, 0.0, i2)
    rows_real = jnp.where(imaginary, i2 - i1, r1 + r2)
    rows_imag = jnp.where(imaginary, r1 - r2, i1 + i2)
    return rows_real, rows_imag


def plane(part, spin, color):
    s1, s2 = divmod(spin, 4)
    c1, c2 = divmod(color, 3)
    return part * 144 + ((s1 * 3 + c1) * 4 + s2) * 3 + c2


def spin_products(field, products):
    load = lambda part, spin: [field[plane(part, spin, color)] for color in range(COLORS)]

    def chain(terms):
        total = None
        for left, right in terms:
            product = left.astype(F32) * right.astype(F32)
            total = product if total is None else total + product
        return total

    row = 0
    for lo in range(SPINS):
        lo_real, lo_imag = load(0, lo), load(1, lo)
        lo_minus = [-value for value in lo_real]
        for hi in range(lo + 1, SPINS):
            hi_real, hi_imag = load(0, hi), load(1, hi)
            real = chain([*zip(lo_real, hi_real), *zip(lo_imag, hi_imag)])
            imag = chain([*zip(lo_imag, hi_real), *zip(lo_minus, hi_imag)])
            products[row : row + 16] = jnp.concatenate([real, imag], axis=0).astype(BF16)
            row += 16
    for first in range(0, SPINS, 2):
        squares = []
        for spin in (first, first + 1):
            real, imag = load(0, spin), load(1, spin)
            squares.append(chain([*zip(real, real), *zip(imag, imag)]))
        products[row : row + 16] = jnp.concatenate(squares, axis=0).astype(BF16)
        row += 16


def peer(gx, dx, dc):
    core = lax.rem(gx, 2)
    return lax.rem(gx // 2 + dx, 4) * 2 + core + dc - 2 * dc * core


OFFSETS = [(dx, dc) for dx in (2, 1, 3, 0) for dc in (1, 0)]


def front_kernel(
    prop, gamma_hbm, table_hbm, wz_hbm, received,
    field, gamma, table, wz, spread, weights, products, message, load_sem, small_sem, ready_sem, go_sem, send_sem, recv_sem,
):
    gx, gy = lax.axis_index("gx"), lax.axis_index("gy")
    me = gx * 4 + gy
    small = [
        pltpu.make_async_copy(source, target, small_sem.at[i])
        for i, (source, target) in enumerate([(gamma_hbm, gamma), (table_hbm, table), (wz_hbm, wz)])
    ]

    def load(j):
        start = j * LANES if isinstance(j, int) else pl.multiple_of(j * LANES, LANES)
        return pltpu.make_async_copy(prop.at[:, :, pl.ds(start, LANES)], field.at[j], load_sem.at[j])

    small[0].start()
    small[1].start()
    load(0).start()
    small[2].start()
    for j in range(1, BLOCKS):
        load(j).start()
    barrier = pltpu.get_barrier_semaphore()

    def each_peer(rows, act):
        for dx, dc in OFFSETS:
            for to_y in rows:
                if (dx, dc) == (0, 0):
                    pl.when(gy != to_y)(functools.partial(act, gx, to_y))
                else:
                    act(peer(gx, dx, dc), to_y)

    def greet(to_x, to_y):
        pl.semaphore_signal(barrier, inc=1, device_id={"gx": to_x, "gy": to_y}, device_id_type=MESH)

    early = gy < 2

    @pl.when(early)
    def _():
        each_peer(EARLY + LATE, greet)

    @pl.when(jnp.logical_not(early))
    def _():
        pl.semaphore_wait(barrier, 16)
        each_peer(
            EARLY,
            lambda to_x, to_y: pl.semaphore_signal(
                ready_sem, inc=1, device_id={"gx": to_x, "gy": to_y}, device_id_type=MESH
            ),
        )

    spread[...] = jnp.zeros_like(spread)
    slot = lax.div(lax.broadcasted_iota(jnp.int32, (32, LANES), 1), 8)
    spread[256:288] = jnp.where(
        slot == lax.broadcasted_iota(jnp.int32, (32, LANES), 0), 1.0, 0.0
    ).astype(BF16)
    small[0].wait()
    small[1].wait()
    rows = jnp.concatenate([gamma[...].astype(F32), jnp.zeros((8, 112), F32)], axis=1)
    rows = jnp.concatenate([rows, jnp.zeros((120, 128), F32)], axis=0)
    channels = jnp.transpose(rows)[:CHANNELS, :8].astype(jnp.int32)

    slot_rows = jnp.concatenate(channel_rows(channels, table[...]), axis=0).astype(BF16)
    keep = lax.broadcasted_iota(jnp.int32, (8, LANES), 0) == lax.rem(
        lax.broadcasted_iota(jnp.int32, (8, LANES), 1), 8
    )
    for tile in range(8):
        rows = jnp.dot(slot_rows, spread[256 - 32 * tile : 512 - 32 * tile], preferred_element_type=F32)
        for row in range(0, 32, 2):
            pair = [
                jnp.where(keep, jnp.broadcast_to(rows[row + i : row + i + 1], (8, LANES)), 0.0)
                for i in range(2)
            ]
            weights[row * 8 : row * 8 + 16, tile * LANES : (tile + 1) * LANES] = jnp.concatenate(
                pair, axis=0
            ).astype(BF16)
    small[2].wait()

    def block(j, carry):
        load(j).wait()
        spin_products(field.at[j], products)
        density = jnp.dot(weights[...], products[...], preferred_element_type=F32).astype(BF16)
        pieces = [
            jnp.concatenate(
                [density[:128, t * 128 : t * 128 + 128], density[128:, t * 128 : t * 128 + 128]], axis=1
            )
            for t in range(2)
        ]
        along = lax.dot_general(
            wz[...], jnp.concatenate(pieces, axis=0), (((1,), (1,)), ((), ())), preferred_element_type=F32
        )
        along = along.reshape(32, 8, LANES)
        message[:, j] = jnp.concatenate([along[:, :, :128], along[:, :, 128:]], axis=1).astype(BF16)
        received[me * BLOCKS + j] = message[me, j]

        @pl.when(jnp.logical_and(j == 0, early))
        def _():
            pl.semaphore_wait(barrier, 15)

        each_peer(
            EARLY,
            lambda to_x, to_y: send(
                message.at[to_x * 4 + to_y, j], received.at[me * BLOCKS + j], to_x, to_y
            ),
        )
        return carry

    def send(source, target, to_x, to_y):
        pltpu.make_async_remote_copy(
            src_ref=source,
            dst_ref=target,
            send_sem=send_sem,
            recv_sem=recv_sem,
            device_id={"gx": to_x, "gy": to_y},
            device_id_type=MESH,
        ).start()

    lax.fori_loop(0, BLOCKS, block, 0)

    @pl.when(early)
    def _():
        pl.semaphore_wait(ready_sem, 16)
        pl.semaphore_signal(go_sem, inc=1, device_id={"gx": gx, "gy": gy + 2}, device_id_type=MESH)

    @pl.when(jnp.logical_not(early))
    def _():
        pl.semaphore_wait(go_sem, 1)

    each_peer(
        LATE,
        lambda to_x, to_y: send(
            message.at[to_x * 4 + to_y], received.at[pl.ds(me * BLOCKS, BLOCKS)], to_x, to_y
        ),
    )
    remote = pl.ds(0, 31 * BLOCKS)
    everything = received.at[remote]
    pltpu.make_async_copy(everything, everything, send_sem).wait()
    pltpu.make_async_copy(everything, everything, recv_sem).wait()


def back_kernel(received, wy, wx, out, along_y, spectrum, out_sem):
    for gx in range(8):
        piece = received[gx * 16 : gx * 16 + 16].reshape(256, 128)
        turned = lax.dot_general(piece, wy[...], (((0,), (0,)), ((), ())), preferred_element_type=F32)
        along_y[gx] = turned.reshape(CHANNELS, 8, 512)
    for g in range(CHANNELS):
        rows = along_y[:, g].reshape(EXTENT, 512)
        rows = jnp.concatenate([rows[:, :256], rows[:, 256:]], axis=0).astype(BF16)
        both = jnp.dot(wx[...], rows, preferred_element_type=F32)
        spectrum[g, 0] = both[:, :128]
        spectrum[g, 1] = both[:, 128:]
        pltpu.make_async_copy(spectrum.at[g], out.at[g], out_sem.at[g]).start()
    for g in range(CHANNELS):
        pltpu.make_async_copy(spectrum.at[g], out.at[g], out_sem.at[g]).wait()


def body(propagator, gamma_table):
    vmem = pl.BlockSpec(memory_space=pltpu.VMEM)
    hbm = pl.BlockSpec(memory_space=pltpu.HBM)
    prop = propagator.reshape(288, 8, 1024)
    received = pl.pallas_call(
        front_kernel,
        out_shape=pltpu.VMEM((128, 16, 128), BF16),
        in_specs=[hbm, hbm, hbm, hbm],
        out_specs=vmem,
        scratch_shapes=[
            pltpu.VMEM((BLOCKS, 288, 8, LANES), BF16),
            pltpu.VMEM((8, CHANNELS), jnp.int32),
            pltpu.VMEM((8, 256), jnp.int32),
            pltpu.VMEM((256, 256), BF16),
            pltpu.VMEM((512, LANES), BF16),
            pltpu.VMEM((256, 2048), BF16),
            pltpu.VMEM((2048, LANES), BF16),
            pltpu.VMEM((32, BLOCKS, 16, 128), BF16),
            pltpu.SemaphoreType.DMA((BLOCKS,)),
            pltpu.SemaphoreType.DMA((3,)),
            pltpu.SemaphoreType.REGULAR,
            pltpu.SemaphoreType.REGULAR,
            pltpu.SemaphoreType.DMA,
            pltpu.SemaphoreType.DMA,
        ],
        compiler_params=pltpu.CompilerParams(
            collective_id=0, has_side_effects=True, vmem_limit_bytes=FRONT_VMEM
        ),
    )(*[pltpu.with_memory_space_constraint(x, pltpu.HBM) for x in (prop, gamma_table.T, jnp.asarray(slot_table()), jnp.asarray(weights_z(), BF16))])
    out = pl.pallas_call(
        back_kernel,
        out_shape=jax.ShapeDtypeStruct((CHANNELS, 2, EXTENT, 128), F32),
        in_specs=[vmem, vmem, vmem],
        out_specs=hbm,
        scratch_shapes=[
            pltpu.VMEM((8, CHANNELS, 8, 512), F32),
            pltpu.VMEM((CHANNELS, 2, EXTENT, 128), F32),
            pltpu.SemaphoreType.DMA((CHANNELS,)),
        ],
        compiler_params=pltpu.CompilerParams(vmem_limit_bytes=BACK_VMEM),
    )(received, jnp.asarray(weights_y(), BF16), jnp.asarray(weights_x(), BF16))
    return out[None]


def solution(mesh):
    return jax.shard_map(
        body,
        mesh=mesh,
        in_specs=(P("ta", None, None, None, None, None, "gx", "gy"), P()),
        out_specs=P("ta", None, ("gx", "gy"), None, None),
        check_vma=False,
    )
```

```python
import functools
import math

import jax
import jax.numpy as jnp
import numpy as np
from jax import lax
from jax.experimental import pallas as pl
from jax.experimental.pallas import tpu as pltpu
from jax.sharding import PartitionSpec as P

EXTENT = 64
CHANNELS = 16
SPINS = 16
COLORS = 9
BLOCKS = 4
LANES = 256
EARLY, LATE = (0, 1), (3, 2)
PARCELS = ((0, 0), (1, 1), (2, 3))
FRONT_VMEM = 20 * 2**20
BACK_VMEM = 16 * 2**20
MESH = pl.DeviceIdType.MESH
F32 = jnp.float32
BF16 = jnp.bfloat16
PAIRS = [(lo, hi) for lo in range(SPINS) for hi in range(lo + 1, SPINS)]


def slot_table():
    slots = [(lo, hi, part) for lo, hi in PAIRS for part in (0, 1)]
    slots += [(spin, spin, 0) for spin in range(SPINS)]
    table = np.zeros((8, 256), np.int32)
    table[:3] = np.array(slots, np.int32).T
    return table


def dft_tables():
    steps = np.arange(EXTENT)
    angles = (steps[:, None] * steps[None, :] % EXTENT) * (2.0 * math.pi / EXTENT)
    norm = 1.0 / math.sqrt(EXTENT)
    return np.cos(angles) * norm, np.sin(angles) * norm


def rotation(cosine, sine):
    table = np.zeros((2, EXTENT, 2, EXTENT))
    table[0, :, 0] = cosine
    table[1, :, 0] = sine
    table[0, :, 1] = -sine
    table[1, :, 1] = cosine
    return table


def weights_z():
    turn = rotation(*dft_tables())
    table = np.zeros((32, 2, 2, 2, 2, 2, EXTENT))
    for y in range(2):
        block = turn.transpose(3, 2, 0, 1).reshape(32, 2, 2, 2, EXTENT)
        table[:, :, :, y, :, y, :] = block
    return table.reshape(256, 256)


def weights_y():
    turn = rotation(*dft_tables()).reshape(2, 4, 4, 2, 2, 2, EXTENT)
    table = np.zeros((4, 4, 2, 2, 2, 2, 2, 2, EXTENT))
    for kz in range(2):
        table[:, :, :, kz, :, :, kz] = turn.transpose(1, 2, 3, 0, 4, 5, 6)
    return table.reshape(256, 256)


def weights_x():
    cosine, sine = dft_tables()
    return np.concatenate([cosine.T, sine.T], axis=1)


def channel_rows(gamma, table):
    lo, hi = table[0:1], table[1:2]
    imaginary = table[2:3] == 1

    def pick(base, index):
        out = jnp.zeros((CHANNELS, index.shape[1]), jnp.int32)
        for spin in range(4):
            out = jnp.where(index == spin, gamma[:, base + spin : base + spin + 1], out)
        return out

    lo_1, lo_2 = lax.div(lo, 4), lax.rem(lo, 4)
    hi_1, hi_2 = lax.div(hi, 4), lax.rem(hi, 4)
    phase = {}
    for name, (s1, s2, s3, s4) in {
        "straight": (lo_1, lo_2, hi_1, hi_2),
        "reversed": (hi_1, hi_2, lo_1, lo_2),
    }.items():
        hit = jnp.logical_and(pick(0, s3) == s1, pick(0, s2) == s4)
        turn = jnp.where(hit, lax.rem(pick(4, s3) + pick(4, s2), 4), 7)
        one, zero = jnp.float32(1), jnp.float32(0)
        real = jnp.where(turn == 0, one, zero) - jnp.where(turn == 2, one, zero)
        imag = jnp.where(turn == 1, one, zero) - jnp.where(turn == 3, one, zero)
        phase[name] = (real, imag)
    (r1, i1), (r2, i2) = phase["straight"], phase["reversed"]
    diagonal = lo == hi
    r2 = jnp.where(diagonal, 0.0, r2)
    i2 = jnp.where(diagonal, 0.0, i2)
    rows_real = jnp.where(imaginary, i2 - i1, r1 + r2)
    rows_imag = jnp.where(imaginary, r1 - r2, i1 + i2)
    return rows_real, rows_imag


def plane(part, spin, color):
    s1, s2 = divmod(spin, 4)
    c1, c2 = divmod(color, 3)
    return part * 144 + ((s1 * 3 + c1) * 4 + s2) * 3 + c2


def spin_products(field, products):
    load = lambda part, spin: [field[plane(part, spin, color)] for color in range(COLORS)]

    def chain(terms):
        total = None
        for left, right in terms:
            product = left.astype(F32) * right.astype(F32)
            total = product if total is None else total + product
        return total

    row = 0
    for lo in range(SPINS):
        lo_real, lo_imag = load(0, lo), load(1, lo)
        lo_minus = [-value for value in lo_real]
        for hi in range(lo + 1, SPINS):
            hi_real, hi_imag = load(0, hi), load(1, hi)
            real = chain([*zip(lo_real, hi_real), *zip(lo_imag, hi_imag)])
            imag = chain([*zip(lo_imag, hi_real), *zip(lo_minus, hi_imag)])
            products[row : row + 16] = jnp.concatenate([real, imag], axis=0).astype(BF16)
            row += 16
    for first in range(0, SPINS, 2):
        squares = []
        for spin in (first, first + 1):
            real, imag = load(0, spin), load(1, spin)
            squares.append(chain([*zip(real, real), *zip(imag, imag)]))
        products[row : row + 16] = jnp.concatenate(squares, axis=0).astype(BF16)
        row += 16


def peer(gx, dx, dc):
    core = lax.rem(gx, 2)
    return lax.rem(gx // 2 + dx, 4) * 2 + core + dc - 2 * dc * core


OFFSETS = [(dx, dc) for dx in (2, 1, 3, 0) for dc in (1, 0)]


def front_kernel(
    prop, gamma_hbm, table_hbm, wz_hbm, received,
    field, gamma, table, wz, spread, weights, products, message, load_sem, small_sem, ready_sem, go_sem, send_sem, recv_sem,
):
    gx, gy = lax.axis_index("gx"), lax.axis_index("gy")
    me = gx * 4 + gy
    small = [
        pltpu.make_async_copy(source, target, small_sem.at[i])
        for i, (source, target) in enumerate([(gamma_hbm, gamma), (table_hbm, table), (wz_hbm, wz)])
    ]

    def load(j):
        start = j * LANES if isinstance(j, int) else pl.multiple_of(j * LANES, LANES)
        return pltpu.make_async_copy(prop.at[:, :, pl.ds(start, LANES)], field.at[j], load_sem.at[j])

    small[0].start()
    small[1].start()
    load(0).start()
    small[2].start()
    barrier = pltpu.get_barrier_semaphore()

    def each_peer(rows, act):
        for dx, dc in OFFSETS:
            for to_y in rows:
                if (dx, dc) == (0, 0):
                    pl.when(gy != to_y)(functools.partial(act, gx, to_y))
                else:
                    act(peer(gx, dx, dc), to_y)

    def greet(to_x, to_y):
        pl.semaphore_signal(barrier, inc=1, device_id={"gx": to_x, "gy": to_y}, device_id_type=MESH)

    early = gy < 2

    @pl.when(early)
    def _():
        each_peer(EARLY + LATE, greet)

    @pl.when(jnp.logical_not(early))
    def _():
        pl.semaphore_wait(barrier, 16)
        each_peer(
            EARLY,
            lambda to_x, to_y: pl.semaphore_signal(
                ready_sem, inc=1, device_id={"gx": to_x, "gy": to_y}, device_id_type=MESH
            ),
        )

    spread[...] = jnp.zeros_like(spread)
    slot = lax.div(lax.broadcasted_iota(jnp.int32, (32, LANES), 1), 8)
    spread[256:288] = jnp.where(
        slot == lax.broadcasted_iota(jnp.int32, (32, LANES), 0), 1.0, 0.0
    ).astype(BF16)
    small[0].wait()
    small[1].wait()
    rows = jnp.concatenate([gamma[...].astype(F32), jnp.zeros((8, 112), F32)], axis=1)
    rows = jnp.concatenate([rows, jnp.zeros((120, 128), F32)], axis=0)
    channels = jnp.transpose(rows)[:CHANNELS, :8].astype(jnp.int32)

    slot_rows = jnp.concatenate(channel_rows(channels, table[...]), axis=0).astype(BF16)
    keep = lax.broadcasted_iota(jnp.int32, (8, LANES), 0) == lax.rem(
        lax.broadcasted_iota(jnp.int32, (8, LANES), 1), 8
    )
    for tile in range(8):
        rows = jnp.dot(slot_rows, spread[256 - 32 * tile : 512 - 32 * tile], preferred_element_type=F32)
        for row in range(0, 32, 2):
            pair = [
                jnp.where(keep, jnp.broadcast_to(rows[row + i : row + i + 1], (8, LANES)), 0.0)
                for i in range(2)
            ]
            weights[row * 8 : row * 8 + 16, tile * LANES : (tile + 1) * LANES] = jnp.concatenate(
                pair, axis=0
            ).astype(BF16)
    small[2].wait()

    def block(j, carry):
        load(j).wait()
        pl.when(j < BLOCKS - 1)(lambda: load(j + 1).start())
        spin_products(field.at[j], products)
        density = jnp.dot(weights[...], products[...], preferred_element_type=F32).astype(BF16)
        pieces = [
            jnp.concatenate(
                [density[:128, t * 128 : t * 128 + 128], density[128:, t * 128 : t * 128 + 128]], axis=1
            )
            for t in range(2)
        ]
        along = lax.dot_general(
            wz[...], jnp.concatenate(pieces, axis=0), (((1,), (1,)), ((), ())), preferred_element_type=F32
        )
        along = along.reshape(32, 8, LANES)
        message[:, j] = jnp.concatenate([along[:, :, :128], along[:, :, 128:]], axis=1).astype(BF16)
        received[me * BLOCKS + j] = message[me, j]

        @pl.when(jnp.logical_and(j == 0, early))
        def _():
            pl.semaphore_wait(barrier, 15)

        for first, last in PARCELS:
            pl.when(j == last)(functools.partial(send_blocks, first, last + 1 - first))
        return carry

    def send_blocks(first, count):
        each_peer(
            EARLY,
            lambda to_x, to_y: send(
                message.at[to_x * 4 + to_y, pl.ds(first, count)],
                received.at[pl.ds(me * BLOCKS + first, count)],
                to_x,
                to_y,
            ),
        )

    def send(source, target, to_x, to_y):
        pltpu.make_async_remote_copy(
            src_ref=source,
            dst_ref=target,
            send_sem=send_sem,
            recv_sem=recv_sem,
            device_id={"gx": to_x, "gy": to_y},
            device_id_type=MESH,
        ).start()

    lax.fori_loop(0, BLOCKS, block, 0)

    @pl.when(early)
    def _():
        pl.semaphore_wait(ready_sem, 16)
        pl.semaphore_signal(go_sem, inc=1, device_id={"gx": gx, "gy": gy + 2}, device_id_type=MESH)

    @pl.when(jnp.logical_not(early))
    def _():
        pl.semaphore_wait(go_sem, 1)

    each_peer(
        LATE,
        lambda to_x, to_y: send(
            message.at[to_x * 4 + to_y], received.at[pl.ds(me * BLOCKS, BLOCKS)], to_x, to_y
        ),
    )
    remote = pl.ds(0, 31 * BLOCKS)
    everything = received.at[remote]
    pltpu.make_async_copy(everything, everything, send_sem).wait()
    pltpu.make_async_copy(everything, everything, recv_sem).wait()


def back_kernel(received, wy, wx, out, along_y, spectrum, out_sem):
    for gx in range(8):
        piece = received[gx * 16 : gx * 16 + 16].reshape(256, 128)
        turned = lax.dot_general(piece, wy[...], (((0,), (0,)), ((), ())), preferred_element_type=F32)
        along_y[gx] = turned.reshape(CHANNELS, 8, 256)
    sign = jnp.where(lax.broadcasted_iota(jnp.int32, (EXTENT, 128), 1) < EXTENT, 1.0, -1.0)
    for g in range(CHANNELS):
        rows = along_y[:, g].reshape(EXTENT, 256)
        swapped = [pltpu.roll(rows[:, kz * 128 : kz * 128 + 128], EXTENT, 1) * sign for kz in range(2)]
        rows = jnp.concatenate([rows, jnp.concatenate(swapped, axis=1)], axis=0).astype(BF16)
        both = jnp.dot(wx[...], rows, preferred_element_type=F32)
        spectrum[g, 0] = both[:, :128]
        spectrum[g, 1] = both[:, 128:]
        pltpu.make_async_copy(spectrum.at[g], out.at[g], out_sem.at[g]).start()
    for g in range(CHANNELS):
        pltpu.make_async_copy(spectrum.at[g], out.at[g], out_sem.at[g]).wait()


def body(propagator, gamma_table):
    vmem = pl.BlockSpec(memory_space=pltpu.VMEM)
    hbm = pl.BlockSpec(memory_space=pltpu.HBM)
    prop = propagator.reshape(288, 8, 1024)
    received = pl.pallas_call(
        front_kernel,
        out_shape=pltpu.VMEM((128, 16, 128), BF16),
        in_specs=[hbm, hbm, hbm, hbm],
        out_specs=vmem,
        scratch_shapes=[
            pltpu.VMEM((BLOCKS, 288, 8, LANES), BF16),
            pltpu.VMEM((8, CHANNELS), jnp.int32),
            pltpu.VMEM((8, 256), jnp.int32),
            pltpu.VMEM((256, 256), BF16),
            pltpu.VMEM((512, LANES), BF16),
            pltpu.VMEM((256, 2048), BF16),
            pltpu.VMEM((2048, LANES), BF16),
            pltpu.VMEM((32, BLOCKS, 16, 128), BF16),
            pltpu.SemaphoreType.DMA((BLOCKS,)),
            pltpu.SemaphoreType.DMA((3,)),
            pltpu.SemaphoreType.REGULAR,
            pltpu.SemaphoreType.REGULAR,
            pltpu.SemaphoreType.DMA,
            pltpu.SemaphoreType.DMA,
        ],
        compiler_params=pltpu.CompilerParams(
            collective_id=0, has_side_effects=True, vmem_limit_bytes=FRONT_VMEM
        ),
    )(*[pltpu.with_memory_space_constraint(x, pltpu.HBM) for x in (prop, gamma_table.T, jnp.asarray(slot_table()), jnp.asarray(weights_z(), BF16))])
    out = pl.pallas_call(
        back_kernel,
        out_shape=jax.ShapeDtypeStruct((CHANNELS, 2, EXTENT, 128), F32),
        in_specs=[vmem, vmem, vmem],
        out_specs=hbm,
        scratch_shapes=[
            pltpu.VMEM((8, CHANNELS, 8, 256), F32),
            pltpu.VMEM((CHANNELS, 2, EXTENT, 128), F32),
            pltpu.SemaphoreType.DMA((CHANNELS,)),
        ],
        compiler_params=pltpu.CompilerParams(vmem_limit_bytes=BACK_VMEM),
    )(received, jnp.asarray(weights_y(), BF16), jnp.asarray(weights_x(), BF16))
    return out[None]


def solution(mesh):
    return jax.shard_map(
        body,
        mesh=mesh,
        in_specs=(P("ta", None, None, None, None, None, "gx", "gy"), P()),
        out_specs=P("ta", None, ("gx", "gy"), None, None),
        check_vma=False,
    )
```

```python
import functools
import math

import jax
import jax.numpy as jnp
import numpy as np
from jax import lax
from jax.experimental import pallas as pl
from jax.experimental.pallas import tpu as pltpu
from jax.sharding import PartitionSpec as P

EXTENT = 64
CHANNELS = 16
SPINS = 16
COLORS = 9
BLOCKS = 4
LANES = 256
EARLY, LATE = (0, 1), (3, 2)
PARCELS = ((0, 0), (1, 1), (2, 3))
FRONT_VMEM = 20 * 2**20
BACK_VMEM = 16 * 2**20
MESH = pl.DeviceIdType.MESH
F32 = jnp.float32
BF16 = jnp.bfloat16
PAIRS = [(lo, hi) for lo in range(SPINS) for hi in range(lo + 1, SPINS)]


def slot_table():
    slots = [(lo, hi, part) for lo, hi in PAIRS for part in (0, 1)]
    slots += [(spin, spin, 0) for spin in range(SPINS)]
    table = np.zeros((8, 256), np.int32)
    table[:3] = np.array(slots, np.int32).T
    return table


def dft_tables():
    steps = np.arange(EXTENT)
    angles = (steps[:, None] * steps[None, :] % EXTENT) * (2.0 * math.pi / EXTENT)
    norm = 1.0 / math.sqrt(EXTENT)
    return np.cos(angles) * norm, np.sin(angles) * norm


def rotation(cosine, sine):
    table = np.zeros((2, EXTENT, 2, EXTENT))
    table[0, :, 0] = cosine
    table[1, :, 0] = sine
    table[0, :, 1] = -sine
    table[1, :, 1] = cosine
    return table


def weights_z():
    turn = rotation(*dft_tables())
    table = np.zeros((32, 2, 2, 2, 2, 2, EXTENT))
    for y in range(2):
        block = turn.transpose(3, 2, 0, 1).reshape(32, 2, 2, 2, EXTENT)
        table[:, :, :, y, :, y, :] = block
    return table.reshape(256, 256)


def weights_y():
    turn = rotation(*dft_tables()).reshape(2, 4, 4, 2, 2, 2, EXTENT)
    table = np.zeros((4, 4, 2, 2, 2, 2, 2, 2, EXTENT))
    for kz in range(2):
        table[:, :, :, kz, :, :, kz] = turn.transpose(1, 2, 3, 0, 4, 5, 6)
    return table.reshape(256, 256)


def weights_x():
    cosine, sine = dft_tables()
    return np.concatenate([cosine.T, sine.T], axis=1)


def channel_rows(gamma, table):
    lo, hi = table[0:1], table[1:2]
    imaginary = table[2:3] == 1

    def pick(base, index):
        out = jnp.zeros((CHANNELS, index.shape[1]), jnp.int32)
        for spin in range(4):
            out = jnp.where(index == spin, gamma[:, base + spin : base + spin + 1], out)
        return out

    lo_1, lo_2 = lax.div(lo, 4), lax.rem(lo, 4)
    hi_1, hi_2 = lax.div(hi, 4), lax.rem(hi, 4)
    phase = {}
    for name, (s1, s2, s3, s4) in {
        "straight": (lo_1, lo_2, hi_1, hi_2),
        "reversed": (hi_1, hi_2, lo_1, lo_2),
    }.items():
        hit = jnp.logical_and(pick(0, s3) == s1, pick(0, s2) == s4)
        turn = jnp.where(hit, lax.rem(pick(4, s3) + pick(4, s2), 4), 7)
        one, zero = jnp.float32(1), jnp.float32(0)
        real = jnp.where(turn == 0, one, zero) - jnp.where(turn == 2, one, zero)
        imag = jnp.where(turn == 1, one, zero) - jnp.where(turn == 3, one, zero)
        phase[name] = (real, imag)
    (r1, i1), (r2, i2) = phase["straight"], phase["reversed"]
    diagonal = lo == hi
    r2 = jnp.where(diagonal, 0.0, r2)
    i2 = jnp.where(diagonal, 0.0, i2)
    rows_real = jnp.where(imaginary, i2 - i1, r1 + r2)
    rows_imag = jnp.where(imaginary, r1 - r2, i1 + i2)
    return rows_real, rows_imag


def plane(part, spin, color):
    s1, s2 = divmod(spin, 4)
    c1, c2 = divmod(color, 3)
    return part * 144 + ((s1 * 3 + c1) * 4 + s2) * 3 + c2


def spin_products(field, products):
    load = lambda part, spin: [field[plane(part, spin, color)] for color in range(COLORS)]

    def chain(terms):
        total = None
        for left, right in terms:
            product = left.astype(F32) * right.astype(F32)
            total = product if total is None else total + product
        return total

    row = 0
    for lo in range(SPINS):
        lo_real, lo_imag = load(0, lo), load(1, lo)
        lo_minus = [-value for value in lo_real]
        for hi in range(lo + 1, SPINS):
            hi_real, hi_imag = load(0, hi), load(1, hi)
            real = chain([*zip(lo_real, hi_real), *zip(lo_imag, hi_imag)])
            imag = chain([*zip(lo_imag, hi_real), *zip(lo_minus, hi_imag)])
            products[row : row + 16] = jnp.concatenate([real, imag], axis=0).astype(BF16)
            row += 16
    for first in range(0, SPINS, 2):
        squares = []
        for spin in (first, first + 1):
            real, imag = load(0, spin), load(1, spin)
            squares.append(chain([*zip(real, real), *zip(imag, imag)]))
        products[row : row + 16] = jnp.concatenate(squares, axis=0).astype(BF16)
        row += 16


def peer(gx, dx, dc):
    core = lax.rem(gx, 2)
    return lax.rem(gx // 2 + dx, 4) * 2 + core + dc - 2 * dc * core


OFFSETS = [(dx, dc) for dx in (2, 1, 3, 0) for dc in (1, 0)]


def front_kernel(
    prop, gamma_hbm, table_hbm, wz_hbm, received,
    field, gamma, table, wz, spread, weights, products, message, load_sem, small_sem, ready_sem, go_sem, send_sem, recv_sem,
):
    gx, gy = lax.axis_index("gx"), lax.axis_index("gy")
    me = gx * 4 + gy
    small = [
        pltpu.make_async_copy(source, target, small_sem.at[i])
        for i, (source, target) in enumerate([(gamma_hbm, gamma), (table_hbm, table), (wz_hbm, wz)])
    ]

    def load(j):
        start = j * LANES if isinstance(j, int) else pl.multiple_of(j * LANES, LANES)
        return pltpu.make_async_copy(prop.at[:, :, pl.ds(start, LANES)], field.at[j], load_sem.at[j])

    small[0].start()
    small[1].start()
    load(0).start()
    small[2].start()
    barrier = pltpu.get_barrier_semaphore()

    def each_peer(rows, act):
        for dx, dc in OFFSETS:
            for to_y in rows:
                if (dx, dc) == (0, 0):
                    pl.when(gy != to_y)(functools.partial(act, gx, to_y))
                else:
                    act(peer(gx, dx, dc), to_y)

    def greet(to_x, to_y):
        pl.semaphore_signal(barrier, inc=1, device_id={"gx": to_x, "gy": to_y}, device_id_type=MESH)

    early = gy < 2

    @pl.when(early)
    def _():
        each_peer(EARLY + LATE, greet)

    @pl.when(jnp.logical_not(early))
    def _():
        pl.semaphore_wait(barrier, 16)
        each_peer(
            EARLY,
            lambda to_x, to_y: pl.semaphore_signal(
                ready_sem, inc=1, device_id={"gx": to_x, "gy": to_y}, device_id_type=MESH
            ),
        )

    spread[...] = jnp.zeros_like(spread)
    slot = lax.div(lax.broadcasted_iota(jnp.int32, (32, LANES), 1), 8)
    spread[256:288] = jnp.where(
        slot == lax.broadcasted_iota(jnp.int32, (32, LANES), 0), 1.0, 0.0
    ).astype(BF16)
    small[0].wait()
    small[1].wait()
    rows = jnp.concatenate([gamma[...].astype(F32), jnp.zeros((8, 112), F32)], axis=1)
    rows = jnp.concatenate([rows, jnp.zeros((120, 128), F32)], axis=0)
    channels = jnp.transpose(rows)[:CHANNELS, :8].astype(jnp.int32)

    slot_rows = jnp.concatenate(channel_rows(channels, table[...]), axis=0).astype(BF16)
    keep = lax.broadcasted_iota(jnp.int32, (8, LANES), 0) == lax.rem(
        lax.broadcasted_iota(jnp.int32, (8, LANES), 1), 8
    )
    for tile in range(8):
        rows = jnp.dot(slot_rows, spread[256 - 32 * tile : 512 - 32 * tile], preferred_element_type=F32)
        for row in range(0, 32, 2):
            pair = [
                jnp.where(keep, jnp.broadcast_to(rows[row + i : row + i + 1], (8, LANES)), 0.0)
                for i in range(2)
            ]
            weights[row * 8 : row * 8 + 16, tile * LANES : (tile + 1) * LANES] = jnp.concatenate(
                pair, axis=0
            ).astype(BF16)
    small[2].wait()

    def block(j, carry):
        load(j).wait()
        pl.when(j < BLOCKS - 1)(lambda: load(j + 1).start())
        spin_products(field.at[j], products)
        density = jnp.dot(weights[...], products[...], preferred_element_type=F32).astype(BF16)
        pieces = [
            jnp.concatenate(
                [density[:128, t * 128 : t * 128 + 128], density[128:, t * 128 : t * 128 + 128]], axis=1
            )
            for t in range(2)
        ]
        along = lax.dot_general(
            wz[...], jnp.concatenate(pieces, axis=0), (((1,), (1,)), ((), ())), preferred_element_type=F32
        )
        along = along.reshape(32, 8, LANES)
        message[:, j] = jnp.concatenate([along[:, :, :128], along[:, :, 128:]], axis=1).astype(BF16)
        received[me * BLOCKS + j] = message[me, j]

        @pl.when(jnp.logical_and(j == 0, early))
        def _():
            pl.semaphore_wait(barrier, 15)

        for first, last in PARCELS:
            pl.when(j == last)(functools.partial(send_blocks, first, last + 1 - first))
        return carry

    def send_blocks(first, count):
        for row in EARLY:
            each_peer(
                (row,),
                lambda to_x, to_y: send(
                    message.at[to_x * 4 + to_y, pl.ds(first, count)],
                    received.at[pl.ds(me * BLOCKS + first, count)],
                    to_x,
                    to_y,
                ),
            )

    def send(source, target, to_x, to_y):
        pltpu.make_async_remote_copy(
            src_ref=source,
            dst_ref=target,
            send_sem=send_sem,
            recv_sem=recv_sem,
            device_id={"gx": to_x, "gy": to_y},
            device_id_type=MESH,
        ).start()

    lax.fori_loop(0, BLOCKS, block, 0)

    @pl.when(early)
    def _():
        pl.semaphore_wait(ready_sem, 16)
        pl.semaphore_signal(go_sem, inc=1, device_id={"gx": gx, "gy": gy + 2}, device_id_type=MESH)

    @pl.when(jnp.logical_not(early))
    def _():
        pl.semaphore_wait(go_sem, 1)

    each_peer(
        LATE,
        lambda to_x, to_y: send(
            message.at[to_x * 4 + to_y], received.at[pl.ds(me * BLOCKS, BLOCKS)], to_x, to_y
        ),
    )
    remote = pl.ds(0, 31 * BLOCKS)
    everything = received.at[remote]
    pltpu.make_async_copy(everything, everything, send_sem).wait()
    pltpu.make_async_copy(everything, everything, recv_sem).wait()


def back_kernel(received, wy, wx, out, along_y, spectrum, out_sem):
    for gx in range(8):
        piece = received[gx * 16 : gx * 16 + 16].reshape(256, 128)
        turned = lax.dot_general(piece, wy[...], (((0,), (0,)), ((), ())), preferred_element_type=F32)
        along_y[gx] = turned.reshape(CHANNELS, 8, 256)
    sign = jnp.where(lax.broadcasted_iota(jnp.int32, (EXTENT, 128), 1) < EXTENT, 1.0, -1.0)
    for g in range(CHANNELS):
        rows = along_y[:, g].reshape(EXTENT, 256)
        swapped = [pltpu.roll(rows[:, kz * 128 : kz * 128 + 128], EXTENT, 1) * sign for kz in range(2)]
        rows = jnp.concatenate([rows, jnp.concatenate(swapped, axis=1)], axis=0).astype(BF16)
        both = jnp.dot(wx[...], rows, preferred_element_type=F32)
        spectrum[g, 0] = both[:, :128]
        spectrum[g, 1] = both[:, 128:]
        pltpu.make_async_copy(spectrum.at[g], out.at[g], out_sem.at[g]).start()
    for g in range(CHANNELS):
        pltpu.make_async_copy(spectrum.at[g], out.at[g], out_sem.at[g]).wait()


def body(propagator, gamma_table):
    vmem = pl.BlockSpec(memory_space=pltpu.VMEM)
    hbm = pl.BlockSpec(memory_space=pltpu.HBM)
    prop = propagator.reshape(288, 8, 1024)
    received = pl.pallas_call(
        front_kernel,
        out_shape=pltpu.VMEM((128, 16, 128), BF16),
        in_specs=[hbm, hbm, hbm, hbm],
        out_specs=vmem,
        scratch_shapes=[
            pltpu.VMEM((BLOCKS, 288, 8, LANES), BF16),
            pltpu.VMEM((8, CHANNELS), jnp.int32),
            pltpu.VMEM((8, 256), jnp.int32),
            pltpu.VMEM((256, 256), BF16),
            pltpu.VMEM((512, LANES), BF16),
            pltpu.VMEM((256, 2048), BF16),
            pltpu.VMEM((2048, LANES), BF16),
            pltpu.VMEM((32, BLOCKS, 16, 128), BF16),
            pltpu.SemaphoreType.DMA((BLOCKS,)),
            pltpu.SemaphoreType.DMA((3,)),
            pltpu.SemaphoreType.REGULAR,
            pltpu.SemaphoreType.REGULAR,
            pltpu.SemaphoreType.DMA,
            pltpu.SemaphoreType.DMA,
        ],
        compiler_params=pltpu.CompilerParams(
            collective_id=0, has_side_effects=True, vmem_limit_bytes=FRONT_VMEM
        ),
    )(*[pltpu.with_memory_space_constraint(x, pltpu.HBM) for x in (prop, gamma_table.T, jnp.asarray(slot_table()), jnp.asarray(weights_z(), BF16))])
    out = pl.pallas_call(
        back_kernel,
        out_shape=jax.ShapeDtypeStruct((CHANNELS, 2, EXTENT, 128), F32),
        in_specs=[vmem, vmem, vmem],
        out_specs=hbm,
        scratch_shapes=[
            pltpu.VMEM((8, CHANNELS, 8, 256), F32),
            pltpu.VMEM((CHANNELS, 2, EXTENT, 128), F32),
            pltpu.SemaphoreType.DMA((CHANNELS,)),
        ],
        compiler_params=pltpu.CompilerParams(vmem_limit_bytes=BACK_VMEM),
    )(received, jnp.asarray(weights_y(), BF16), jnp.asarray(weights_x(), BF16))
    return out[None]


def solution(mesh):
    return jax.shard_map(
        body,
        mesh=mesh,
        in_specs=(P("ta", None, None, None, None, None, "gx", "gy"), P()),
        out_specs=P("ta", None, ("gx", "gy"), None, None),
        check_vma=False,
    )
```
